32 devices in a mesh: grp: 4 (over z), blk: 8 (over y, x, core).
Axes of the slice: x: 2, y: 2, z: 4, core: 2. Of those that a mesh axis runs over, the one named last changes fastest.
Arguments:
- partials: bfloat16 [4, 512, 3584], P('grp', 'blk'), may hold values from -450 to 450
- slot_of_block: int32 [7], replicated, may hold values from 0 to 7, as said below
- stat_left: float32 [8, 512, 512], P('blk'), may hold values from -1 to 257, as said below
- stat_right: float32 [8, 512, 512], P('blk'), may hold values from -1 to 257, as said below
- root_left: bfloat16 [8, 512, 512], P('blk'), may hold values from -0.2 to 2.2, as said below
- root_right: bfloat16 [8, 512, 512], P('blk'), may hold values from -0.2 to 2.2, as said below
Outputs:
- new_left: float32 [8, 512, 512], P('blk')
- new_right: float32 [8, 512, 512], P('blk')
- update: bfloat16 [512, 3584], P('blk')
The draws below stay inside these ranges and needn't reach their ends.
Inputs may be any that keep to these rules, and one draw needn't show every extreme that they name: `slot_of_block`: the 7 owners are distinct. `stat_left`: symmetric. `stat_right`: symmetric. `root_left`: symmetric. `root_right`: symmetric.
All inputs are finite; a program needn't handle non-finite values.
Results may differ from the reference program's by a relative error of at most 0.02.
Values may be sent and summed in bfloat16 or wider, within the bound.
A program may use at most 64 MiB of HBM per device.

```python
import math
import jax
import jax.numpy as jnp
from jax import lax

BLOCK = 512
BLOCKS = 7
COLS = 3584
N_GRP = 4
N_BLK = 8


def draw_partials(key, part):
    key_row, key_col, key_val = jax.random.split(jax.random.fold_in(key, 11), 3)
    positions = jnp.arange(BLOCK, dtype=jnp.float32)
    rising = 3.0 ** (positions / (BLOCK - 1))
    col_scale = jnp.exp(jax.random.uniform(key_col, (COLS,), jnp.float32, 0.0, math.log(10.0)))
    row_scale = rising * jnp.exp(jax.random.uniform(key_row, (BLOCK,), jnp.float32, 0.0, math.log(3.0)))
    values = jax.random.truncated_normal(key_val, -4.0, 4.0, (N_GRP, BLOCK, COLS), jnp.float32)
    return (values * row_scale[None, :, None] * col_scale[None, None, :]).astype(jnp.bfloat16)


def draw_slot_of_block(key, part):
    return jax.random.permutation(jax.random.fold_in(key, 23), N_BLK)[:BLOCKS].astype(jnp.int32)


def symmetric_stat(key):
    key_diag, key_off = jax.random.split(key)
    diagonal = jnp.exp(jax.random.uniform(key_diag, (N_BLK, BLOCK), jnp.float32, math.log(BLOCK / 20.0), math.log(BLOCK / 2.0)))
    noise = jax.random.uniform(key_off, (N_BLK, BLOCK, BLOCK), jnp.float32, -1.0, 1.0)
    noise = 0.5 * (noise + jnp.swapaxes(noise, 1, 2))
    return noise + diagonal[:, :, None] * jnp.eye(BLOCK, dtype=jnp.float32)[None]


def symmetric_root(key):
    key_diag, key_off = jax.random.split(key)
    diagonal = jnp.exp(jax.random.uniform(key_diag, (N_BLK, BLOCK), jnp.float32, math.log(0.5), math.log(2.0)))
    spread = 0.3 / math.sqrt(BLOCK)
    noise = jax.random.truncated_normal(key_off, -3.0, 3.0, (N_BLK, BLOCK, BLOCK), jnp.float32) * spread
    noise = 0.5 * (noise + jnp.swapaxes(noise, 1, 2))
    return noise + diagonal[:, :, None] * jnp.eye(BLOCK, dtype=jnp.float32)[None]


def draw_stat_left(key, part):
    return symmetric_stat(jax.random.fold_in(key, 31))


def draw_stat_right(key, part):
    return symmetric_stat(jax.random.fold_in(key, 37))


def draw_root_left(key, part):
    return symmetric_root(jax.random.fold_in(key, 41)).astype(jnp.bfloat16)


def draw_root_right(key, part):
    return symmetric_root(jax.random.fold_in(key, 43)).astype(jnp.bfloat16)


def setup_inputs(seed: int = 0) -> dict:
    streams_of = jax.random.split(jax.random.key(seed), 7)
    return {
        "partials": draw_partials(jax.random.fold_in(streams_of[6], 71), 0),
        "slot_of_block": draw_slot_of_block(jax.random.fold_in(streams_of[6], 71), 0),
        "stat_left": draw_stat_left(jax.random.fold_in(streams_of[6], 71), 0),
        "stat_right": draw_stat_right(jax.random.fold_in(streams_of[6], 71), 0),
        "root_left": draw_root_left(jax.random.fold_in(streams_of[6], 71), 0),
        "root_right": draw_root_right(jax.random.fold_in(streams_of[6], 71), 0),
    }


def reference(partials, slot_of_block, stat_left, stat_right, root_left, root_right):
    gradient = lax.optimization_barrier(jnp.sum(partials.astype(jnp.float32), axis=0)).astype(jnp.bfloat16)
    widened = gradient.astype(jnp.float32)
    squares = jnp.sum(widened * widened)
    norm_limit = math.sqrt(BLOCK * COLS)
    norm_factor = norm_limit / jnp.sqrt(squares)
    gradient_tiles = gradient.reshape(BLOCK, BLOCKS, BLOCK).transpose(1, 0, 2)
    slot_ids = jnp.arange(N_BLK, dtype=jnp.int32)
    block_ids = jnp.arange(BLOCKS, dtype=jnp.int32)

    def per_slot(inputs):
        slot, left_stat, right_stat, left_root, right_root = inputs
        matches = slot_of_block == slot
        chosen_index = jnp.sum(jnp.where(matches, block_ids, 0)).astype(jnp.int32)
        chosen = lax.dynamic_index_in_dim(gradient_tiles, chosen_index, 0, keepdims=False)
        owned_tile = jnp.where(jnp.any(matches), chosen, jnp.zeros_like(chosen))
        left_gram = jnp.dot(owned_tile, owned_tile.T, preferred_element_type=jnp.float32)
        right_gram = jnp.dot(owned_tile.T, owned_tile, preferred_element_type=jnp.float32)
        factor_sq = norm_factor * norm_factor
        next_left = 0.9 * left_stat + 0.1 * factor_sq * left_gram
        next_right = 0.9 * right_stat + 0.1 * factor_sq * right_gram
        halfway = jnp.dot(left_root, owned_tile, preferred_element_type=jnp.float32).astype(jnp.bfloat16)
        direction = jnp.dot(halfway, right_root, preferred_element_type=jnp.float32)
        owned_wide = owned_tile.astype(jnp.float32)
        grad_norm = jnp.sqrt(jnp.sum(owned_wide * owned_wide))
        dir_norm = jnp.sqrt(jnp.sum(direction * direction) + 1e-06)
        grafted = (norm_factor * grad_norm / dir_norm * direction).astype(jnp.bfloat16)
        return (next_left, next_right, grafted)
    new_left, new_right, grafted = lax.map(per_slot, (slot_ids, stat_left, stat_right, root_left, root_right))
    update = grafted[slot_of_block].transpose(1, 0, 2).reshape(BLOCK, COLS)
    return (new_left, new_right, update)
```

```python
import functools
import math

import jax
import jax.numpy as jnp
from jax import lax
from jax.experimental import pallas as pl
from jax.experimental.pallas import tpu as pltpu
from jax.sharding import PartitionSpec as P

MESH = pl.DeviceIdType.MESH
beta_two = 0.9


def partner(me, k, count):
    if count & (count - 1):
        return lax.rem(me + k, count)
    total, bit = 0, 1
    while bit < count:
        total = total + lax.rem(me // bit + k // bit, 2) * bit
        bit *= 2
    return total


def kernel(
    n_grp, n_blk, slot_ref, x_ref, sl_ref, sr_ref, rl_ref, rr_ref, nl_ref, nr_ref, up_ref,
    xb, snd, rz, tile, dirs, ret, st_out, st_in, scales, sl, sr, rl, rr,
    x_sem, w_sem, a_send, z_recv, b_send, p_send, p_recv, d_send, d_recv, s_send, s_recv,
):
    grp, blk = lax.axis_index("grp"), lax.axis_index("blk")
    n_tiles = xb.shape[0] - 1
    rows, block = xb.shape[1], xb.shape[2]
    half = n_grp // 2
    low = grp < half
    step = jnp.where(low, 1, -1)
    depth = jnp.where(low, half - 1 - grp, grp - half)
    is_mid = depth == 0
    is_end = depth == half - 1
    inner = grp + step
    outer = jnp.where(is_end, grp, grp - step)
    lag = jnp.where(is_end, n_blk, jnp.minimum(2 + 3 * depth, n_blk))

    def x_copy(b):
        cols = pl.ds(pl.multiple_of(b * block, block), block)
        return pltpu.make_async_copy(x_ref.at[0, :, cols], xb.at[b], x_sem.at[b])

    def x_start(b, c):
        x_copy(b).start()
        return c

    def x_wait(b, c):
        x_copy(b).wait()
        return c

    lax.fori_loop(0, n_tiles, x_start, 0)
    w_pairs = ((rl_ref, rl), (rr_ref, rr), (sl_ref, sl), (sr_ref, sr))
    w_copies = [
        pltpu.make_async_copy(src.at[0], dst, w_sem.at[i]) for i, (src, dst) in enumerate(w_pairs)
    ]
    for c in w_copies:
        c.start()

    barrier = pltpu.get_barrier_semaphore()

    def greet(k, c):
        pl.semaphore_signal(
            barrier, inc=1, device_id=(grp, partner(blk, k, n_blk)), device_id_type=MESH
        )
        return c

    pl.semaphore_signal(barrier, inc=1, device_id=(inner, blk), device_id_type=MESH)

    @pl.when(jnp.logical_not(is_end))
    def _():
        pl.semaphore_signal(barrier, inc=1, device_id=(outer, blk), device_id_type=MESH)

    lax.fori_loop(1, n_blk, greet, 0)
    xb[n_tiles] = jnp.zeros((rows, block), xb.dtype)
    lax.fori_loop(0, n_tiles, x_wait, 0)
    pl.semaphore_wait(barrier, n_blk + jnp.where(is_end, 0, 1))

    kind = jnp.where(is_mid, 1, 0)

    def target(t):
        return partner(blk, lax.rem(t + 1, n_blk), n_blk)

    def copy_in(s):
        return pltpu.make_async_remote_copy(
            snd.at[s], rz.at[kind, s], a_send.at[s], z_recv.at[kind, s],
            device_id=(inner, blk), device_id_type=MESH,
        )

    def copy_out(s):
        return pltpu.make_async_remote_copy(
            rz.at[1, s], rz.at[1, s], b_send.at[s], z_recv.at[1, s],
            device_id=(outer, blk), device_id_type=MESH,
        )

    def arrived(k, s):
        return pltpu.make_async_remote_copy(
            rz.at[k, s], rz.at[k, s], a_send.at[s], z_recv.at[k, s],
            device_id=(inner, blk), device_id_type=MESH,
        )

    def copy_tile(s):
        return pltpu.make_async_remote_copy(
            rz.at[1, s], tile.at[blk], p_send.at[s], p_recv.at[blk],
            device_id=(grp, s), device_id_type=MESH,
        )

    def phase(t, c):
        @pl.when(t < n_blk)
        def _():
            s = target(t)
            b = n_tiles
            for i in range(n_tiles):
                b = jnp.where(slot_ref[i] == s, i, b)

            @pl.when(is_end)
            def _():
                snd[s] = xb[b]

            @pl.when(jnp.logical_not(is_end))
            def _():
                arrived(0, s).wait_recv()
                snd[s] = (xb[b].astype(jnp.float32) + rz[0, s].astype(jnp.float32)).astype(snd.dtype)

            copy_in(s).start()

        @pl.when(jnp.logical_and(t >= lag, t < n_blk + lag))
        def _():
            s = target(t - lag)
            arrived(1, s).wait_recv()

            @pl.when(is_mid)
            def _():
                rz[1, s] = (snd[s].astype(jnp.float32) + rz[1, s].astype(jnp.float32)).astype(rz.dtype)

            @pl.when(jnp.logical_not(is_end))
            def _():
                copy_out(s).start()

            @pl.when(t - lag < n_blk - 1)
            def _():
                copy_tile(s).start()

        return c

    lax.fori_loop(0, 2 * n_blk, phase, 0)
    tile[blk] = rz[1, blk]

    def tile_wait(k, c):
        j = partner(blk, k, n_blk)
        pltpu.make_async_remote_copy(
            rz.at[1, j], tile.at[j], p_send.at[j], p_recv.at[j],
            device_id=(grp, j), device_id_type=MESH,
        ).wait_recv()
        return c

    lax.fori_loop(1, n_blk, tile_wait, 0)
    w_copies[0].wait()
    w_copies[1].wait()

    owned = tile[...].reshape(n_blk * rows, block)
    halfway = jnp.dot(rl[...], owned, preferred_element_type=jnp.float32).astype(jnp.bfloat16)
    direction = jnp.dot(halfway, rr[...], preferred_element_type=jnp.float32)
    dirs[...] = direction.astype(dirs.dtype).reshape(n_blk, rows, block)

    def copy_dir(j):
        return pltpu.make_async_remote_copy(
            dirs.at[j], ret.at[blk], d_send.at[j], d_recv.at[blk],
            device_id=(grp, j), device_id_type=MESH,
        )

    def copy_stat(j):
        return pltpu.make_async_remote_copy(
            st_out, st_in.at[blk], s_send.at[j], s_recv.at[blk],
            device_id=(grp, j), device_id_type=MESH,
        )

    wide = owned.astype(jnp.float32)
    own_sq = jnp.sum(wide * wide)
    dir_sq = jnp.sum(direction * direction)
    row_id = lax.broadcasted_iota(jnp.int32, st_out.shape, 0)
    stats = jnp.where(row_id == 0, own_sq, dir_sq)
    st_out[...] = stats
    st_in[blk] = stats

    def stat_start(k, c):
        copy_stat(partner(blk, k, n_blk)).start()
        return c

    def dir_start(k, c):
        copy_dir(partner(blk, n_blk - k, n_blk)).start()
        return c

    lax.fori_loop(1, n_blk, stat_start, 0)
    lax.fori_loop(1, n_blk, dir_start, 0)
    ret[blk] = dirs[blk]

    nl_ref[0] = lax.dot_general(
        owned, owned, (((1,), (1,)), ((), ())), preferred_element_type=jnp.float32
    )
    nr_ref[0] = lax.dot_general(
        owned, owned, (((0,), (0,)), ((), ())), preferred_element_type=jnp.float32
    )

    def stat_wait(k, c):
        j = partner(blk, k, n_blk)
        pltpu.make_async_remote_copy(
            st_out, st_in.at[j], s_send.at[j], s_recv.at[j],
            device_id=(grp, j), device_id_type=MESH,
        ).wait()
        return c

    lax.fori_loop(1, n_blk, stat_wait, 0)
    squares = jnp.zeros((1, st_out.shape[1]), jnp.float32)
    for j in range(n_blk):
        squares = squares + st_in[j, 0:1, :]
    norm_factor = math.sqrt(block * n_tiles * block) / jnp.sqrt(squares)
    for j in range(n_blk):
        scales[j] = norm_factor * jnp.sqrt(st_in[j, 0:1, :]) / jnp.sqrt(st_in[j, 1:2, :] + 1e-6)
    gain = (1.0 - beta_two) * (norm_factor * norm_factor)[:, 0:1]
    w_copies[2].wait()
    w_copies[3].wait()
    nl_ref[0] = beta_two * sl[...] + gain * nl_ref[0]
    nr_ref[0] = beta_two * sr[...] + gain * nr_ref[0]

    def dir_wait(k, c):
        j = partner(blk, k, n_blk)
        pltpu.make_async_remote_copy(
            dirs.at[j], ret.at[j], d_send.at[j], d_recv.at[j],
            device_id=(grp, j), device_id_type=MESH,
        ).wait()
        return c

    lax.fori_loop(1, n_blk, dir_wait, 0)
    for b in range(n_tiles):
        s = slot_ref[b]
        up_ref[:, b * block : (b + 1) * block] = (
            ret[s].astype(jnp.float32) * scales[s][:, 0:1]
        ).astype(up_ref.dtype)

    def drain(s, c):
        copy_in(s).wait_send()

        @pl.when(jnp.logical_not(is_end))
        def _():
            copy_out(s).wait_send()

        @pl.when(s != blk)
        def _():
            copy_tile(s).wait_send()

        return c

    lax.fori_loop(0, n_blk, drain, 0)


def shards(n_grp, n_blk, partials, slot_of_block, stat_left, stat_right, root_left, root_right):
    rows, cols = partials.shape[1], partials.shape[2]
    block = stat_left.shape[1]
    n_tiles = cols // block
    vmem = pltpu.VMEM
    dma = pltpu.SemaphoreType.DMA
    half, single = jnp.bfloat16, jnp.float32
    any_spec = pl.BlockSpec(memory_space=pl.ANY)
    vmem_spec = pl.BlockSpec(memory_space=vmem)
    slots = (n_blk, rows, block)
    return pl.pallas_call(
        functools.partial(kernel, n_grp, n_blk),
        out_shape=(
            jax.ShapeDtypeStruct((1, block, block), single),
            jax.ShapeDtypeStruct((1, block, block), single),
            jax.ShapeDtypeStruct((rows, cols), half),
        ),
        in_specs=[pl.BlockSpec(memory_space=pltpu.SMEM)] + [any_spec] * 5,
        out_specs=(vmem_spec,) * 3,
        scratch_shapes=[
            vmem((n_tiles + 1, rows, block), half),
            vmem(slots, half),
            vmem((2, *slots), half),
            vmem(slots, half),
            vmem(slots, half),
            vmem(slots, half),
            vmem((8, 128), single),
            vmem((n_blk, 8, 128), single),
            vmem((n_blk, 1, 128), single),
            vmem((block, block), single),
            vmem((block, block), single),
            vmem((block, block), half),
            vmem((block, block), half),
            dma((n_tiles,)),
            dma((4,)),
            dma((n_blk,)),
            dma((2, n_blk)),
            dma((n_blk,)),
            dma((n_blk,)),
            dma((n_blk,)),
            dma((n_blk,)),
            dma((n_blk,)),
            dma((n_blk,)),
            dma((n_blk,)),
        ],
        compiler_params=pltpu.CompilerParams(collective_id=0, has_side_effects=True),
        name="shampoo",
    )(slot_of_block, partials, stat_left, stat_right, root_left, root_right)


def solution(mesh):
    return jax.shard_map(
        functools.partial(shards, mesh.shape["grp"], mesh.shape["blk"]),
        mesh=mesh,
        in_specs=(
            P("grp", "blk", None),
            P(),
            P("blk", None, None),
            P("blk", None, None),
            P("blk", None, None),
            P("blk", None, None),
        ),
        out_specs=(P("blk", None, None), P("blk", None, None), P("blk", None)),
        check_vma=False,
    )
```

```python
import functools
import math

import jax
import jax.numpy as jnp
from jax import lax
from jax.experimental import pallas as pl
from jax.experimental.pallas import tpu as pltpu
from jax.sharding import PartitionSpec as P

MESH = pl.DeviceIdType.MESH
beta_two = 0.9
vmem_bytes = 67043328


def partner(me, k, count):
    if count & (count - 1):
        return lax.rem(me + k, count)
    total, bit = 0, 1
    while bit < count:
        total = total + lax.rem(me // bit + k // bit, 2) * bit
        bit *= 2
    return total


def kernel(
    n_grp, n_blk, slot_ref, x_ref, sl_ref, sr_ref, rl_ref, rr_ref, nl_ref, nr_ref, up_ref,
    xb, snd, rz, tile, dirs, ret, st_out, st_in, scales, sl, sr, rl, rr,
    x_sem, w_sem, a_send, z_recv, b_send, p_send, p_recv, d_send, d_recv, s_send, s_recv,
):
    grp, blk = lax.axis_index("grp"), lax.axis_index("blk")
    n_tiles = xb.shape[0] - 1
    rows, block = xb.shape[1], xb.shape[2]
    half = n_grp // 2
    low = grp < half
    step = jnp.where(low, 1, -1)
    depth = jnp.where(low, half - 1 - grp, grp - half)
    is_mid = depth == 0
    is_end = depth == half - 1
    inner = grp + step
    outer = jnp.where(is_end, grp, grp - step)
    lag = jnp.where(is_end, n_blk, jnp.minimum(2 + 3 * depth, n_blk))

    def x_copy(b):
        cols = pl.ds(pl.multiple_of(b * block, block), block)
        return pltpu.make_async_copy(x_ref.at[0, :, cols], xb.at[b], x_sem.at[b])

    def x_start(b, c):
        x_copy(b).start()
        return c

    def x_wait(b, c):
        x_copy(b).wait()
        return c

    lax.fori_loop(0, n_tiles, x_start, 0)
    w_pairs = ((rl_ref, rl), (rr_ref, rr), (sl_ref, sl), (sr_ref, sr))
    w_copies = [
        pltpu.make_async_copy(src.at[0], dst, w_sem.at[i]) for i, (src, dst) in enumerate(w_pairs)
    ]
    for c in w_copies:
        c.start()

    barrier = pltpu.get_barrier_semaphore()

    def greet(k, c):
        pl.semaphore_signal(
            barrier, inc=1, device_id=(grp, partner(blk, k, n_blk)), device_id_type=MESH
        )
        return c

    pl.semaphore_signal(barrier, inc=1, device_id=(inner, blk), device_id_type=MESH)

    @pl.when(jnp.logical_not(is_end))
    def _():
        pl.semaphore_signal(barrier, inc=1, device_id=(outer, blk), device_id_type=MESH)

    lax.fori_loop(1, n_blk, greet, 0)
    xb[n_tiles] = jnp.zeros((rows, block), xb.dtype)
    lax.fori_loop(0, n_tiles, x_wait, 0)
    pl.semaphore_wait(barrier, n_blk + jnp.where(is_end, 0, 1))

    kind = jnp.where(is_mid, 1, 0)

    def target(t):
        return partner(blk, lax.rem(t + 1, n_blk), n_blk)

    def copy_in(s):
        return pltpu.make_async_remote_copy(
            snd.at[s], rz.at[kind, s], a_send.at[s], z_recv.at[kind, s],
            device_id=(inner, blk), device_id_type=MESH,
        )

    def copy_out(s):
        return pltpu.make_async_remote_copy(
            rz.at[1, s], rz.at[1, s], b_send.at[s], z_recv.at[1, s],
            device_id=(outer, blk), device_id_type=MESH,
        )

    def arrived(k, s):
        return pltpu.make_async_remote_copy(
            rz.at[k, s], rz.at[k, s], a_send.at[s], z_recv.at[k, s],
            device_id=(inner, blk), device_id_type=MESH,
        )

    def copy_tile(s):
        return pltpu.make_async_remote_copy(
            rz.at[1, s], tile.at[blk], p_send.at[s], p_recv.at[blk],
            device_id=(grp, s), device_id_type=MESH,
        )

    def phase(t, c):
        @pl.when(t < n_blk)
        def _():
            s = target(t)
            b = n_tiles
            for i in range(n_tiles):
                b = jnp.where(slot_ref[i] == s, i, b)

            @pl.when(is_end)
            def _():
                snd[s] = xb[b]

            @pl.when(jnp.logical_not(is_end))
            def _():
                arrived(0, s).wait_recv()
                snd[s] = (xb[b].astype(jnp.float32) + rz[0, s].astype(jnp.float32)).astype(snd.dtype)

            copy_in(s).start()

        @pl.when(jnp.logical_and(t >= lag, t < n_blk + lag))
        def _():
            s = target(t - lag)
            arrived(1, s).wait_recv()

            @pl.when(is_mid)
            def _():
                rz[1, s] = (snd[s].astype(jnp.float32) + rz[1, s].astype(jnp.float32)).astype(rz.dtype)

            @pl.when(jnp.logical_not(is_end))
            def _():
                copy_out(s).start()

            @pl.when(t - lag < n_blk - 1)
            def _():
                copy_tile(s).start()

        return c

    lax.fori_loop(0, 2 * n_blk, phase, 0)
    tile[blk] = rz[1, blk]

    def tile_wait(k, c):
        j = partner(blk, k, n_blk)
        pltpu.make_async_remote_copy(
            rz.at[1, j], tile.at[j], p_send.at[j], p_recv.at[j],
            device_id=(grp, j), device_id_type=MESH,
        ).wait_recv()
        return c

    lax.fori_loop(1, n_blk, tile_wait, 0)
    w_copies[0].wait()
    w_copies[1].wait()

    owned = tile[...].reshape(n_blk * rows, block)
    halfway = jnp.dot(rl[...], owned, preferred_element_type=jnp.float32).astype(jnp.bfloat16)
    direction = jnp.dot(halfway, rr[...], preferred_element_type=jnp.float32)
    dirs[...] = direction.astype(dirs.dtype).reshape(n_blk, rows, block)

    def copy_dir(j):
        return pltpu.make_async_remote_copy(
            dirs.at[j], ret.at[blk], d_send.at[j], d_recv.at[blk],
            device_id=(grp, j), device_id_type=MESH,
        )

    def copy_stat(j):
        return pltpu.make_async_remote_copy(
            st_out, st_in.at[blk], s_send.at[j], s_recv.at[blk],
            device_id=(grp, j), device_id_type=MESH,
        )

    wide = owned.astype(jnp.float32)
    own_sq = jnp.sum(wide * wide)
    dir_sq = jnp.sum(direction * direction)
    row_id = lax.broadcasted_iota(jnp.int32, st_out.shape, 0)
    stats = jnp.where(row_id == 0, own_sq, dir_sq)
    st_out[...] = stats
    st_in[blk] = stats

    def stat_start(k, c):
        copy_stat(partner(blk, k, n_blk)).start()
        return c

    def dir_start(k, c):
        copy_dir(partner(blk, n_blk - k, n_blk)).start()
        return c

    lax.fori_loop(1, n_blk, stat_start, 0)
    lax.fori_loop(1, n_blk, dir_start, 0)
    ret[blk] = dirs[blk]

    nl_ref[0] = lax.dot_general(
        owned, owned, (((1,), (1,)), ((), ())), preferred_element_type=jnp.float32
    )
    nr_ref[0] = lax.dot_general(
        owned, owned, (((0,), (0,)), ((), ())), preferred_element_type=jnp.float32
    )

    def stat_wait(k, c):
        j = partner(blk, k, n_blk)
        pltpu.make_async_remote_copy(
            st_out, st_in.at[j], s_send.at[j], s_recv.at[j],
            device_id=(grp, j), device_id_type=MESH,
        ).wait()
        return c

    lax.fori_loop(1, n_blk, stat_wait, 0)
    squares = jnp.zeros((1, st_out.shape[1]), jnp.float32)
    for j in range(n_blk):
        squares = squares + st_in[j, 0:1, :]
    norm_factor = math.sqrt(block * n_tiles * block) / jnp.sqrt(squares)
    for j in range(n_blk):
        scales[j] = norm_factor * jnp.sqrt(st_in[j, 0:1, :]) / jnp.sqrt(st_in[j, 1:2, :] + 1e-6)
    gain = (1.0 - beta_two) * (norm_factor * norm_factor)[:, 0:1]
    w_copies[2].wait()
    w_copies[3].wait()
    nl_ref[0] = beta_two * sl[...] + gain * nl_ref[0]
    nr_ref[0] = beta_two * sr[...] + gain * nr_ref[0]

    def dir_wait(k, c):
        j = partner(blk, k, n_blk)
        pltpu.make_async_remote_copy(
            dirs.at[j], ret.at[j], d_send.at[j], d_recv.at[j],
            device_id=(grp, j), device_id_type=MESH,
        ).wait()
        return c

    lax.fori_loop(1, n_blk, dir_wait, 0)
    for b in range(n_tiles):
        s = slot_ref[b]
        up_ref[:, b * block : (b + 1) * block] = (
            ret[s].astype(jnp.float32) * scales[s][:, 0:1]
        ).astype(up_ref.dtype)

    def drain(s, c):
        copy_in(s).wait_send()

        @pl.when(jnp.logical_not(is_end))
        def _():
            copy_out(s).wait_send()

        @pl.when(s != blk)
        def _():
            copy_tile(s).wait_send()

        return c

    lax.fori_loop(0, n_blk, drain, 0)


def writer(*refs):
    count = len(refs) // 2
    sources, targets, sems = refs[:count], refs[count:-1], refs[-1]
    copies = [
        pltpu.make_async_copy(src, dst, sems.at[i])
        for i, (src, dst) in enumerate(zip(sources, targets))
    ]
    for c in copies:
        c.start()
    for c in copies:
        c.wait()


def shards(n_grp, n_blk, partials, slot_of_block, stat_left, stat_right, root_left, root_right):
    rows, cols = partials.shape[1], partials.shape[2]
    block = stat_left.shape[1]
    n_tiles = cols // block
    vmem = pltpu.VMEM
    dma = pltpu.SemaphoreType.DMA
    half, single = jnp.bfloat16, jnp.float32
    hbm_spec = pl.BlockSpec(memory_space=pltpu.HBM)
    vmem_spec = pl.BlockSpec(memory_space=vmem)
    slots = (n_blk, rows, block)
    results = (
        ((1, block, block), single),
        ((1, block, block), single),
        ((rows, cols), half),
    )
    held_bytes = sum(math.prod(shape) * jnp.dtype(dtype).itemsize for shape, dtype in results)
    held = pl.pallas_call(
        functools.partial(kernel, n_grp, n_blk),
        out_shape=tuple(vmem(shape, dtype) for shape, dtype in results),
        in_specs=[pl.BlockSpec(memory_space=pltpu.SMEM)] + [hbm_spec] * 5,
        out_specs=(vmem_spec,) * 3,
        scratch_shapes=[
            vmem((n_tiles + 1, rows, block), half),
            vmem(slots, half),
            vmem((2, *slots), half),
            vmem(slots, half),
            vmem(slots, half),
            vmem(slots, half),
            vmem((8, 128), single),
            vmem((n_blk, 8, 128), single),
            vmem((n_blk, 1, 128), single),
            vmem((block, block), single),
            vmem((block, block), single),
            vmem((block, block), half),
            vmem((block, block), half),
            dma((n_tiles,)),
            dma((4,)),
            dma((n_blk,)),
            dma((2, n_blk)),
            dma((n_blk,)),
            dma((n_blk,)),
            dma((n_blk,)),
            dma((n_blk,)),
            dma((n_blk,)),
            dma((n_blk,)),
            dma((n_blk,)),
        ],
        compiler_params=pltpu.CompilerParams(
            collective_id=0, has_side_effects=True, vmem_limit_bytes=vmem_bytes - held_bytes
        ),
        name="shampoo",
    )(slot_of_block, partials, stat_left, stat_right, root_left, root_right)
    return pl.pallas_call(
        writer,
        out_shape=tuple(jax.ShapeDtypeStruct(shape, dtype) for shape, dtype in results),
        in_specs=[vmem_spec] * 3,
        out_specs=(hbm_spec,) * 3,
        scratch_shapes=[dma((3,))],
        compiler_params=pltpu.CompilerParams(vmem_limit_bytes=2**20),
        name="writer",
    )(*held)


def solution(mesh):
    return jax.shard_map(
        functools.partial(shards, mesh.shape["grp"], mesh.shape["blk"]),
        mesh=mesh,
        in_specs=(
            P("grp", "blk", None),
            P(),
            P("blk", None, None),
            P("blk", None, None),
            P("blk", None, None),
            P("blk", None, None),
        ),
        out_specs=(P("blk", None, None), P("blk", None, None), P("blk", None)),
        check_vma=False,
    )
```

```python
import functools
import math

import jax
import jax.numpy as jnp
from jax import lax
from jax.experimental import pallas as pl
from jax.experimental.pallas import tpu as pltpu
from jax.sharding import PartitionSpec as P

MESH = pl.DeviceIdType.MESH
beta_two = 0.9
vmem_bytes = 67043328


def partner(me, k, count):
    if count & (count - 1):
        return lax.rem(me + k, count)
    total, bit = 0, 1
    while bit < count:
        total = total + lax.rem(me // bit + k // bit, 2) * bit
        bit *= 2
    return total


def kernel(
    n_grp, n_blk, slot_ref, x_ref, sl_ref, sr_ref, rl_ref, rr_ref, nl_ref, nr_ref, up_ref,
    xb, snd, rz, tile, dirs, ret, st_out, st_in, scales, sl, sr, rl, rr,
    x_sem, w_sem, a_send, z_recv, b_send, p_send, p_recv, d_send, d_recv, s_send, s_recv,
):
    grp, blk = lax.axis_index("grp"), lax.axis_index("blk")
    n_tiles = xb.shape[0] - 1
    parts, height, block = xb.shape[1], xb.shape[2], xb.shape[3]
    rows = parts * height
    units = n_blk * parts
    groups = 2 if n_blk % 2 == 0 else 1
    fellows = n_blk // groups
    half = n_grp // 2
    low = grp < half
    step = jnp.where(low, 1, -1)
    depth = jnp.where(low, half - 1 - grp, grp - half)
    is_mid = depth == 0
    is_end = depth == half - 1
    inner = grp + step
    outer = jnp.where(is_end, grp, grp - step)
    lag = jnp.where(is_end, units, jnp.minimum((1 + 2 * depth) * 2 * parts, units))
    early = jnp.logical_and(is_end, lax.rem(blk, groups) < groups - 1)
    moment = lag + jnp.where(early, units // groups + 3, units)

    def x_copy(b, h):
        cols = pl.ds(pl.multiple_of(b * block, block), block)
        return pltpu.make_async_copy(
            x_ref.at[0, pl.ds(h * height, height), cols], xb.at[b, h], x_sem.at[b, h]
        )

    def x_start(b, c):
        for h in range(parts):
            x_copy(b, h).start()
        return c

    def x_wait(b, c):
        for h in range(parts):
            x_copy(b, h).wait()
        return c

    lax.fori_loop(0, n_tiles, x_start, 0)
    w_pairs = ((rl_ref, rl), (rr_ref, rr), (sl_ref, sl), (sr_ref, sr))
    w_copies = [
        pltpu.make_async_copy(src.at[0], dst, w_sem.at[i]) for i, (src, dst) in enumerate(w_pairs)
    ]
    for c in w_copies:
        c.start()

    barrier = pltpu.get_barrier_semaphore()

    def greet(k, c):
        pl.semaphore_signal(
            barrier, inc=1, device_id=(grp, partner(blk, k, n_blk)), device_id_type=MESH
        )
        return c

    pl.semaphore_signal(barrier, inc=1, device_id=(inner, blk), device_id_type=MESH)

    @pl.when(jnp.logical_not(is_end))
    def _():
        pl.semaphore_signal(barrier, inc=1, device_id=(outer, blk), device_id_type=MESH)

    lax.fori_loop(1, n_blk, greet, 0)
    xb[n_tiles] = jnp.zeros((parts, height, block), xb.dtype)
    lax.fori_loop(0, n_tiles, x_wait, 0)
    pl.semaphore_wait(barrier, n_blk + jnp.where(is_end, 0, 1))

    kind = jnp.where(is_mid, 1, 0)

    def target(u):
        k = u // parts
        fellow = partner(blk // groups, lax.rem(lax.rem(k, fellows) + 1, fellows), fellows)
        return fellow * groups + k // fellows, lax.rem(u, parts)

    def copy_in(s, h):
        return pltpu.make_async_remote_copy(
            snd.at[s, h], rz.at[kind, s, h], a_send.at[s, h], z_recv.at[kind, s, h],
            device_id=(inner, blk), device_id_type=MESH,
        )

    def copy_out(s, h):
        return pltpu.make_async_remote_copy(
            rz.at[1, s, h], rz.at[1, s, h], b_send.at[s, h], z_recv.at[1, s, h],
            device_id=(outer, blk), device_id_type=MESH,
        )

    def arrived(k, s, h):
        return pltpu.make_async_remote_copy(
            rz.at[k, s, h], rz.at[k, s, h], a_send.at[s, h], z_recv.at[k, s, h],
            device_id=(inner, blk), device_id_type=MESH,
        )

    def copy_tile(s, h):
        return pltpu.make_async_remote_copy(
            rz.at[1, s, h], tile.at[blk, h], p_send.at[s, h], p_recv.at[blk, h],
            device_id=(grp, s), device_id_type=MESH,
        )

    def tile_wait(k, c):
        j = partner(blk, k, n_blk)
        for h in range(parts):
            pltpu.make_async_remote_copy(
                rz.at[1, j, h], tile.at[j, h], p_send.at[j, h], p_recv.at[j, h],
                device_id=(grp, j), device_id_type=MESH,
            ).wait_recv()
        return c

    def copy_dir(j):
        return pltpu.make_async_remote_copy(
            dirs.at[j], ret.at[blk], d_send.at[j], d_recv.at[blk],
            device_id=(grp, j), device_id_type=MESH,
        )

    def copy_stat(j):
        return pltpu.make_async_remote_copy(
            st_out, st_in.at[blk], s_send.at[j], s_recv.at[blk],
            device_id=(grp, j), device_id_type=MESH,
        )

    def stat_start(k, c):
        copy_stat(partner(blk, k, n_blk)).start()
        return c

    def dir_start(k, c):
        copy_dir(partner(blk, n_blk - k, n_blk)).start()
        return c

    def apply():
        lax.fori_loop(1, n_blk, tile_wait, 0)
        w_copies[0].wait()
        w_copies[1].wait()
        mine = tile[...].reshape(n_blk * rows, block)
        halfway = jnp.dot(rl[...], mine, preferred_element_type=jnp.float32).astype(jnp.bfloat16)
        direction = jnp.dot(halfway, rr[...], preferred_element_type=jnp.float32)
        dirs[...] = direction.astype(dirs.dtype).reshape(n_blk, rows, block)
        wide = mine.astype(jnp.float32)
        own_sq = jnp.sum(wide * wide)
        dir_sq = jnp.sum(direction * direction)
        row_id = lax.broadcasted_iota(jnp.int32, st_out.shape, 0)
        stats = jnp.where(row_id == 0, own_sq, dir_sq)
        st_out[...] = stats
        st_in[blk] = stats
        lax.fori_loop(1, n_blk, stat_start, 0)
        lax.fori_loop(1, n_blk, dir_start, 0)
        ret[blk] = dirs[blk]

    def phase(t, c):
        @pl.when(t < units)
        def _():
            s, h = target(t)
            b = n_tiles
            for i in range(n_tiles):
                b = jnp.where(slot_ref[i] == s, i, b)

            @pl.when(is_end)
            def _():
                snd[s, h] = xb[b, h]

            @pl.when(jnp.logical_not(is_end))
            def _():
                arrived(0, s, h).wait_recv()
                total = xb[b, h].astype(jnp.float32) + rz[0, s, h].astype(jnp.float32)
                snd[s, h] = total.astype(snd.dtype)

            copy_in(s, h).start()

        @pl.when(jnp.logical_and(t >= lag, t < units + lag))
        def _():
            s, h = target(t - lag)
            arrived(1, s, h).wait_recv()

            @pl.when(is_mid)
            def _():
                total = snd[s, h].astype(jnp.float32) + rz[1, s, h].astype(jnp.float32)
                rz[1, s, h] = total.astype(rz.dtype)

            @pl.when(jnp.logical_not(is_end))
            def _():
                copy_out(s, h).start()

            @pl.when(s != blk)
            def _():
                copy_tile(s, h).start()

            @pl.when(s == blk)
            def _():
                tile[blk, h] = rz[1, blk, h]

        @pl.when(t == moment)
        def _():
            apply()

        return c

    lax.fori_loop(0, 2 * units + 1, phase, 0)
    owned = tile[...].reshape(n_blk * rows, block)
    nl_ref[0] = lax.dot_general(
        owned, owned, (((1,), (1,)), ((), ())), preferred_element_type=jnp.float32
    )
    nr_ref[0] = lax.dot_general(
        owned, owned, (((0,), (0,)), ((), ())), preferred_element_type=jnp.float32
    )

    def stat_wait(k, c):
        j = partner(blk, k, n_blk)
        pltpu.make_async_remote_copy(
            st_out, st_in.at[j], s_send.at[j], s_recv.at[j],
            device_id=(grp, j), device_id_type=MESH,
        ).wait()
        return c

    lax.fori_loop(1, n_blk, stat_wait, 0)
    squares = jnp.zeros((1, st_out.shape[1]), jnp.float32)
    for j in range(n_blk):
        squares = squares + st_in[j, 0:1, :]
    norm_factor = math.sqrt(block * n_tiles * block) / jnp.sqrt(squares)
    for j in range(n_blk):
        scales[j] = norm_factor * jnp.sqrt(st_in[j, 0:1, :]) / jnp.sqrt(st_in[j, 1:2, :] + 1e-6)
    gain = (1.0 - beta_two) * (norm_factor * norm_factor)[:, 0:1]
    w_copies[2].wait()
    w_copies[3].wait()
    nl_ref[0] = beta_two * sl[...] + gain * nl_ref[0]
    nr_ref[0] = beta_two * sr[...] + gain * nr_ref[0]

    def dir_wait(k, c):
        j = partner(blk, k, n_blk)
        pltpu.make_async_remote_copy(
            dirs.at[j], ret.at[j], d_send.at[j], d_recv.at[j],
            device_id=(grp, j), device_id_type=MESH,
        ).wait()
        return c

    lax.fori_loop(1, n_blk, dir_wait, 0)
    for b in range(n_tiles):
        s = slot_ref[b]
        up_ref[:, b * block : (b + 1) * block] = (
            ret[s].astype(jnp.float32) * scales[s][:, 0:1]
        ).astype(up_ref.dtype)

    def drain(s, c):
        for h in range(parts):
            copy_in(s, h).wait_send()

        @pl.when(jnp.logical_not(is_end))
        def _():
            for h in range(parts):
                copy_out(s, h).wait_send()

        @pl.when(s != blk)
        def _():
            for h in range(parts):
                copy_tile(s, h).wait_send()

        return c

    lax.fori_loop(0, n_blk, drain, 0)


def writer(*refs):
    count = len(refs) // 2
    sources, targets, sems = refs[:count], refs[count:-1], refs[-1]
    copies = [
        pltpu.make_async_copy(src, dst, sems.at[i])
        for i, (src, dst) in enumerate(zip(sources, targets))
    ]
    for c in copies:
        c.start()
    for c in copies:
        c.wait()


def shards(n_grp, n_blk, partials, slot_of_block, stat_left, stat_right, root_left, root_right):
    rows, cols = partials.shape[1], partials.shape[2]
    block = stat_left.shape[1]
    n_tiles = cols // block
    vmem = pltpu.VMEM
    dma = pltpu.SemaphoreType.DMA
    half, single = jnp.bfloat16, jnp.float32
    hbm_spec = pl.BlockSpec(memory_space=pltpu.HBM)
    vmem_spec = pl.BlockSpec(memory_space=vmem)
    parts = 2 if rows % 32 == 0 else 1
    slots = (n_blk, rows, block)
    pieces = (parts, rows // parts, block)
    results = (
        ((1, block, block), single),
        ((1, block, block), single),
        ((rows, cols), half),
    )
    held_bytes = sum(math.prod(shape) * jnp.dtype(dtype).itemsize for shape, dtype in results)
    held = pl.pallas_call(
        functools.partial(kernel, n_grp, n_blk),
        out_shape=tuple(vmem(shape, dtype) for shape, dtype in results),
        in_specs=[pl.BlockSpec(memory_space=pltpu.SMEM)] + [hbm_spec] * 5,
        out_specs=(vmem_spec,) * 3,
        scratch_shapes=[
            vmem((n_tiles + 1, *pieces), half),
            vmem((n_blk, *pieces), half),
            vmem((2, n_blk, *pieces), half),
            vmem((n_blk, *pieces), half),
            vmem(slots, half),
            vmem(slots, half),
            vmem((8, 128), single),
            vmem((n_blk, 8, 128), single),
            vmem((n_blk, 1, 128), single),
            vmem((block, block), single),
            vmem((block, block), single),
            vmem((block, block), half),
            vmem((block, block), half),
            dma((n_tiles, parts)),
            dma((4,)),
            dma((n_blk, parts)),
            dma((2, n_blk, parts)),
            dma((n_blk, parts)),
            dma((n_blk, parts)),
            dma((n_blk, parts)),
            dma((n_blk,)),
            dma((n_blk,)),
            dma((n_blk,)),
            dma((n_blk,)),
        ],
        compiler_params=pltpu.CompilerParams(
            collective_id=0, has_side_effects=True, vmem_limit_bytes=vmem_bytes - held_bytes
        ),
        name="shampoo",
    )(slot_of_block, partials, stat_left, stat_right, root_left, root_right)
    return pl.pallas_call(
        writer,
        out_shape=tuple(jax.ShapeDtypeStruct(shape, dtype) for shape, dtype in results),
        in_specs=[vmem_spec] * 3,
        out_specs=(hbm_spec,) * 3,
        scratch_shapes=[dma((3,))],
        compiler_params=pltpu.CompilerParams(vmem_limit_bytes=2**20),
        name="writer",
    )(*held)


def solution(mesh):
    return jax.shard_map(
        functools.partial(shards, mesh.shape["grp"], mesh.shape["blk"]),
        mesh=mesh,
        in_specs=(
            P("grp", "blk", None),
            P(),
            P("blk", None, None),
            P("blk", None, None),
            P("blk", None, None),
            P("blk", None, None),
        ),
        out_specs=(P("blk", None, None), P("blk", None, None), P("blk", None)),
        check_vma=False,
    )
```

```python
import functools
import math

import jax
import jax.numpy as jnp
from jax import lax
from jax.experimental import pallas as pl
from jax.experimental.pallas import tpu as pltpu
from jax.sharding import PartitionSpec as P

MESH = pl.DeviceIdType.MESH
beta_two = 0.9
vmem_bytes = 67043328


def partner(me, k, count):
    if count & (count - 1):
        return lax.rem(me + k, count)
    total, bit = 0, 1
    while bit < count:
        total = total + lax.rem(me // bit + k // bit, 2) * bit
        bit *= 2
    return total


def kernel(
    n_grp, n_blk, slot_ref, x_ref, sl_ref, sr_ref, rl_ref, rr_ref, nl_ref, nr_ref, up_ref,
    xb, snd, rz, tile, dirs, ret, st_out, st_in, scales, sl, sr, rl, rr,
    x_sem, w_sem, a_send, z_recv, b_send, p_send, p_recv, d_send, d_recv, s_send, s_recv,
):
    grp, blk = lax.axis_index("grp"), lax.axis_index("blk")
    n_tiles = xb.shape[0] - 1
    parts, height, block = xb.shape[1], xb.shape[2], xb.shape[3]
    rows = parts * height
    units = n_blk * parts
    groups = 2 if n_blk % 2 == 0 else 1
    fellows = n_blk // groups
    half = n_grp // 2
    low = grp < half
    step = jnp.where(low, 1, -1)
    depth = jnp.where(low, half - 1 - grp, grp - half)
    is_mid = depth == 0
    is_end = depth == half - 1
    leaf = jnp.logical_and(is_end, half > 1)
    feeder = jnp.logical_and(depth == half - 2, half > 1)
    inner = grp + step
    outer = jnp.where(is_end, grp, grp - step)
    lag = jnp.minimum((1 + 2 * depth) * 2 * parts, units)
    early = lax.rem(blk, groups) < groups - 1
    moment = jnp.where(leaf, units, lag + jnp.where(early, units // groups + 5, units))

    def x_copy(b, h):
        cols = pl.ds(pl.multiple_of(b * block, block), block)
        return pltpu.make_async_copy(
            x_ref.at[0, pl.ds(h * height, height), cols], xb.at[b, h], x_sem.at[b, h]
        )

    def x_start(b, c):
        for h in range(parts):
            x_copy(b, h).start()
        return c

    def x_wait(b, c):
        for h in range(parts):
            x_copy(b, h).wait()
        return c

    lax.fori_loop(0, n_tiles, x_start, 0)
    w_pairs = ((rl_ref, rl), (rr_ref, rr), (sl_ref, sl), (sr_ref, sr))
    w_copies = [
        pltpu.make_async_copy(src.at[0], dst, w_sem.at[i]) for i, (src, dst) in enumerate(w_pairs)
    ]
    for c in w_copies:
        c.start()

    barrier = pltpu.get_barrier_semaphore()

    def greet(k, c):
        pl.semaphore_signal(
            barrier, inc=1, device_id=(grp, partner(blk, k, n_blk)), device_id_type=MESH
        )
        return c

    pl.semaphore_signal(barrier, inc=1, device_id=(inner, blk), device_id_type=MESH)

    @pl.when(jnp.logical_not(is_end))
    def _():
        pl.semaphore_signal(barrier, inc=1, device_id=(outer, blk), device_id_type=MESH)

    @pl.when(jnp.logical_or(leaf, feeder))
    def _():
        def greet_next(k, c):
            pl.semaphore_signal(
                barrier, inc=1, device_id=(jnp.where(leaf, inner, outer), partner(blk, k, n_blk)),
                device_id_type=MESH,
            )
            return c

        lax.fori_loop(1, n_blk, greet_next, 0)

    lax.fori_loop(1, n_blk, greet, 0)
    xb[n_tiles] = jnp.zeros((parts, height, block), xb.dtype)
    lax.fori_loop(0, n_tiles, x_wait, 0)
    next_plane = jnp.where(jnp.logical_or(leaf, feeder), n_blk - 1, 0)
    pl.semaphore_wait(barrier, n_blk + jnp.where(is_end, 0, 1) + next_plane)

    kind = jnp.where(is_mid, 1, 0)

    def target(u):
        k = u // parts
        fellow = partner(blk // groups, lax.rem(lax.rem(k, fellows) + 1, fellows), fellows)
        return fellow * groups + k // fellows, lax.rem(u, parts)

    def copy_in(s, h):
        return pltpu.make_async_remote_copy(
            snd.at[s, h], rz.at[kind, s, h], a_send.at[s, h], z_recv.at[kind, s, h],
            device_id=(inner, blk), device_id_type=MESH,
        )

    def copy_out(s, h):
        return pltpu.make_async_remote_copy(
            rz.at[1, s, h], rz.at[1, s, h], b_send.at[s, h], z_recv.at[1, s, h],
            device_id=(outer, blk), device_id_type=MESH,
        )

    def copy_far(s, h):
        return pltpu.make_async_remote_copy(
            rz.at[1, s, h], tile.at[blk, h], b_send.at[s, h], p_recv.at[blk, h],
            device_id=(outer, s), device_id_type=MESH,
        )

    def arrived(k, s, h):
        return pltpu.make_async_remote_copy(
            rz.at[k, s, h], rz.at[k, s, h], a_send.at[s, h], z_recv.at[k, s, h],
            device_id=(inner, blk), device_id_type=MESH,
        )

    def copy_tile(s, h):
        return pltpu.make_async_remote_copy(
            rz.at[1, s, h], tile.at[blk, h], p_send.at[s, h], p_recv.at[blk, h],
            device_id=(grp, s), device_id_type=MESH,
        )

    def tile_wait(k, c):
        j = partner(blk, k, n_blk)
        for h in range(parts):
            pltpu.make_async_remote_copy(
                rz.at[1, j, h], tile.at[j, h], p_send.at[j, h], p_recv.at[j, h],
                device_id=(grp, j), device_id_type=MESH,
            ).wait_recv()
        return c

    def copy_dir(j):
        return pltpu.make_async_remote_copy(
            dirs.at[j], ret.at[blk], d_send.at[j], d_recv.at[blk],
            device_id=(grp, j), device_id_type=MESH,
        )

    def copy_stat(j):
        return pltpu.make_async_remote_copy(
            st_out, st_in.at[blk], s_send.at[j], s_recv.at[blk],
            device_id=(grp, j), device_id_type=MESH,
        )

    def stat_start(k, c):
        copy_stat(partner(blk, k, n_blk)).start()
        return c

    def dir_start(k, c):
        copy_dir(partner(blk, n_blk - k, n_blk)).start()
        return c

    def apply():
        lax.fori_loop(1, n_blk, tile_wait, 0)

        @pl.when(leaf)
        def _():
            tile_wait(0, 0)

        w_copies[0].wait()
        w_copies[1].wait()
        mine = tile[...].reshape(n_blk * rows, block)
        halfway = jnp.dot(rl[...], mine, preferred_element_type=jnp.float32).astype(jnp.bfloat16)
        direction = jnp.dot(halfway, rr[...], preferred_element_type=jnp.float32)
        dirs[...] = direction.astype(dirs.dtype).reshape(n_blk, rows, block)
        wide = mine.astype(jnp.float32)
        own_sq = jnp.sum(wide * wide)
        dir_sq = jnp.sum(direction * direction)
        row_id = lax.broadcasted_iota(jnp.int32, st_out.shape, 0)
        stats = jnp.where(row_id == 0, own_sq, dir_sq)
        st_out[...] = stats
        st_in[blk] = stats
        lax.fori_loop(1, n_blk, stat_start, 0)
        lax.fori_loop(1, n_blk, dir_start, 0)
        ret[blk] = dirs[blk]

    def phase(t, c):
        @pl.when(t < units)
        def _():
            s, h = target(t)
            b = n_tiles
            for i in range(n_tiles):
                b = jnp.where(slot_ref[i] == s, i, b)

            @pl.when(is_end)
            def _():
                snd[s, h] = xb[b, h]

            @pl.when(jnp.logical_not(is_end))
            def _():
                arrived(0, s, h).wait_recv()
                total = xb[b, h].astype(jnp.float32) + rz[0, s, h].astype(jnp.float32)
                snd[s, h] = total.astype(snd.dtype)

            copy_in(s, h).start()

        @pl.when(jnp.logical_and(jnp.logical_not(leaf), jnp.logical_and(t >= lag, t < units + lag)))
        def _():
            s, h = target(t - lag)
            arrived(1, s, h).wait_recv()

            @pl.when(is_mid)
            def _():
                total = snd[s, h].astype(jnp.float32) + rz[1, s, h].astype(jnp.float32)
                rz[1, s, h] = total.astype(rz.dtype)

            @pl.when(feeder)
            def _():
                copy_far(s, h).start()

            @pl.when(jnp.logical_not(jnp.logical_or(is_end, feeder)))
            def _():
                copy_out(s, h).start()

            @pl.when(s != blk)
            def _():
                copy_tile(s, h).start()

            @pl.when(s == blk)
            def _():
                tile[blk, h] = rz[1, blk, h]

        @pl.when(t == moment)
        def _():
            apply()

        return c

    lax.fori_loop(0, 2 * units + 1, phase, 0)
    owned = tile[...].reshape(n_blk * rows, block)
    nl_ref[0] = lax.dot_general(
        owned, owned, (((1,), (1,)), ((), ())), preferred_element_type=jnp.float32
    )
    nr_ref[0] = lax.dot_general(
        owned, owned, (((0,), (0,)), ((), ())), preferred_element_type=jnp.float32
    )

    def stat_wait(k, c):
        j = partner(blk, k, n_blk)
        pltpu.make_async_remote_copy(
            st_out, st_in.at[j], s_send.at[j], s_recv.at[j],
            device_id=(grp, j), device_id_type=MESH,
        ).wait()
        return c

    lax.fori_loop(1, n_blk, stat_wait, 0)
    squares = jnp.zeros((1, st_out.shape[1]), jnp.float32)
    for j in range(n_blk):
        squares = squares + st_in[j, 0:1, :]
    norm_factor = math.sqrt(block * n_tiles * block) / jnp.sqrt(squares)
    for j in range(n_blk):
        scales[j] = norm_factor * jnp.sqrt(st_in[j, 0:1, :]) / jnp.sqrt(st_in[j, 1:2, :] + 1e-6)
    gain = (1.0 - beta_two) * (norm_factor * norm_factor)[:, 0:1]
    w_copies[2].wait()
    w_copies[3].wait()
    nl_ref[0] = beta_two * sl[...] + gain * nl_ref[0]
    nr_ref[0] = beta_two * sr[...] + gain * nr_ref[0]

    def dir_wait(k, c):
        j = partner(blk, k, n_blk)
        pltpu.make_async_remote_copy(
            dirs.at[j], ret.at[j], d_send.at[j], d_recv.at[j],
            device_id=(grp, j), device_id_type=MESH,
        ).wait()
        return c

    lax.fori_loop(1, n_blk, dir_wait, 0)
    for b in range(n_tiles):
        s = slot_ref[b]
        up_ref[:, b * block : (b + 1) * block] = (
            ret[s].astype(jnp.float32) * scales[s][:, 0:1]
        ).astype(up_ref.dtype)

    def drain(s, c):
        for h in range(parts):
            copy_in(s, h).wait_send()

        @pl.when(jnp.logical_not(is_end))
        def _():
            for h in range(parts):
                copy_out(s, h).wait_send()

        @pl.when(jnp.logical_and(s != blk, jnp.logical_not(leaf)))
        def _():
            for h in range(parts):
                copy_tile(s, h).wait_send()

        return c

    lax.fori_loop(0, n_blk, drain, 0)


def writer(*refs):
    count = len(refs) // 2
    sources, targets, sems = refs[:count], refs[count:-1], refs[-1]
    copies = [
        pltpu.make_async_copy(src, dst, sems.at[i])
        for i, (src, dst) in enumerate(zip(sources, targets))
    ]
    for c in copies:
        c.start()
    for c in copies:
        c.wait()


def shards(n_grp, n_blk, partials, slot_of_block, stat_left, stat_right, root_left, root_right):
    rows, cols = partials.shape[1], partials.shape[2]
    block = stat_left.shape[1]
    n_tiles = cols // block
    vmem = pltpu.VMEM
    dma = pltpu.SemaphoreType.DMA
    half, single = jnp.bfloat16, jnp.float32
    hbm_spec = pl.BlockSpec(memory_space=pltpu.HBM)
    vmem_spec = pl.BlockSpec(memory_space=vmem)
    parts = 2 if rows % 32 == 0 else 1
    slots = (n_blk, rows, block)
    pieces = (parts, rows // parts, block)
    results = (
        ((1, block, block), single),
        ((1, block, block), single),
        ((rows, cols), half),
    )
    held_bytes = sum(math.prod(shape) * jnp.dtype(dtype).itemsize for shape, dtype in results)
    held = pl.pallas_call(
        functools.partial(kernel, n_grp, n_blk),
        out_shape=tuple(vmem(shape, dtype) for shape, dtype in results),
        in_specs=[pl.BlockSpec(memory_space=pltpu.SMEM)] + [hbm_spec] * 5,
        out_specs=(vmem_spec,) * 3,
        scratch_shapes=[
            vmem((n_tiles + 1, *pieces), half),
            vmem((n_blk, *pieces), half),
            vmem((2, n_blk, *pieces), half),
            vmem((n_blk, *pieces), half),
            vmem(slots, half),
            vmem(slots, half),
            vmem((8, 128), single),
            vmem((n_blk, 8, 128), single),
            vmem((n_blk, 1, 128), single),
            vmem((block, block), single),
            vmem((block, block), single),
            vmem((block, block), half),
            vmem((block, block), half),
            dma((n_tiles, parts)),
            dma((4,)),
            dma((n_blk, parts)),
            dma((2, n_blk, parts)),
            dma((n_blk, parts)),
            dma((n_blk, parts)),
            dma((n_blk, parts)),
            dma((n_blk,)),
            dma((n_blk,)),
            dma((n_blk,)),
            dma((n_blk,)),
        ],
        compiler_params=pltpu.CompilerParams(
            collective_id=0, has_side_effects=True, vmem_limit_bytes=vmem_bytes - held_bytes
        ),
        name="shampoo",
    )(slot_of_block, partials, stat_left, stat_right, root_left, root_right)
    return pl.pallas_call(
        writer,
        out_shape=tuple(jax.ShapeDtypeStruct(shape, dtype) for shape, dtype in results),
        in_specs=[vmem_spec] * 3,
        out_specs=(hbm_spec,) * 3,
        scratch_shapes=[dma((3,))],
        compiler_params=pltpu.CompilerParams(vmem_limit_bytes=2**20),
        name="writer",
    )(*held)


def solution(mesh):
    return jax.shard_map(
        functools.partial(shards, mesh.shape["grp"], mesh.shape["blk"]),
        mesh=mesh,
        in_specs=(
            P("grp", "blk", None),
            P(),
            P("blk", None, None),
            P("blk", None, None),
            P("blk", None, None),
            P("blk", None, None),
        ),
        out_specs=(P("blk", None, None), P("blk", None, None), P("blk", None)),
        check_vma=False,
    )
```

```python
import functools
import math

import jax
import jax.numpy as jnp
from jax import lax
from jax.experimental import pallas as pl
from jax.experimental.pallas import tpu as pltpu
from jax.sharding import PartitionSpec as P

MESH = pl.DeviceIdType.MESH
beta_two = 0.9
vmem_bytes = 67043328


def partner(me, k, count):
    if count & (count - 1):
        return lax.rem(me + k, count)
    total, bit = 0, 1
    while bit < count:
        total = total + lax.rem(me // bit + k // bit, 2) * bit
        bit *= 2
    return total


def kernel(
    n_grp, n_blk, slot_ref, x_ref, sl_ref, sr_ref, rl_ref, rr_ref, nl_ref, nr_ref, up_ref,
    xb, snd, rz, tile, dirs, ret, st_out, st_in, scales, sl, sr, rl, rr,
    x_sem, w_sem, a_send, z_recv, b_send, p_send, p_recv, d_send, d_recv, s_send, s_recv,
):
    grp, blk = lax.axis_index("grp"), lax.axis_index("blk")
    n_tiles = xb.shape[0] - 1
    parts, height, block = xb.shape[1], xb.shape[2], xb.shape[3]
    rows = parts * height
    units = n_blk * parts
    groups = 2 if n_blk % 2 == 0 else 1
    fellows = n_blk // groups
    half = n_grp // 2
    low = grp < half
    step = jnp.where(low, 1, -1)
    depth = jnp.where(low, half - 1 - grp, grp - half)
    is_mid = depth == 0
    is_end = depth == half - 1
    leaf = jnp.logical_and(is_end, half > 1)
    feeder = jnp.logical_and(depth == half - 2, half > 1)
    inner = grp + step
    outer = jnp.where(is_end, grp, grp - step)
    lag = jnp.minimum((1 + 2 * depth) * 2 * parts, units)
    moment = jnp.where(leaf, units, lag + units)

    def x_copy(b, h):
        cols = pl.ds(pl.multiple_of(b * block, block), block)
        return pltpu.make_async_copy(
            x_ref.at[0, pl.ds(h * height, height), cols], xb.at[b, h], x_sem.at[b, h]
        )

    def x_start(b, c):
        for h in range(parts):
            x_copy(b, h).start()
        return c

    def x_wait(b, c):
        for h in range(parts):
            x_copy(b, h).wait()
        return c

    lax.fori_loop(0, n_tiles, x_start, 0)
    w_pairs = ((rl_ref, rl), (rr_ref, rr), (sl_ref, sl), (sr_ref, sr))
    w_copies = [
        pltpu.make_async_copy(src.at[0], dst, w_sem.at[i]) for i, (src, dst) in enumerate(w_pairs)
    ]
    for c in w_copies:
        c.start()

    barrier = pltpu.get_barrier_semaphore()

    def greet(k, c):
        pl.semaphore_signal(
            barrier, inc=1, device_id=(grp, partner(blk, k, n_blk)), device_id_type=MESH
        )
        return c

    pl.semaphore_signal(barrier, inc=1, device_id=(inner, blk), device_id_type=MESH)

    @pl.when(jnp.logical_not(is_end))
    def _():
        pl.semaphore_signal(barrier, inc=1, device_id=(outer, blk), device_id_type=MESH)

    @pl.when(jnp.logical_or(leaf, feeder))
    def _():
        def greet_next(k, c):
            pl.semaphore_signal(
                barrier, inc=1, device_id=(jnp.where(leaf, inner, outer), partner(blk, k, n_blk)),
                device_id_type=MESH,
            )
            return c

        lax.fori_loop(1, n_blk, greet_next, 0)

    lax.fori_loop(1, n_blk, greet, 0)
    xb[n_tiles] = jnp.zeros((parts, height, block), xb.dtype)
    lax.fori_loop(0, n_tiles, x_wait, 0)
    next_plane = jnp.where(jnp.logical_or(leaf, feeder), n_blk - 1, 0)
    pl.semaphore_wait(barrier, n_blk + jnp.where(is_end, 0, 1) + next_plane)

    kind = jnp.where(is_mid, 1, 0)

    def target(u):
        k = u // parts
        fellow = partner(blk // groups, lax.rem(lax.rem(k, fellows) + 1, fellows), fellows)
        return fellow * groups + k // fellows, lax.rem(u, parts)

    def copy_in(s, h):
        return pltpu.make_async_remote_copy(
            snd.at[s, h], rz.at[kind, s, h], a_send.at[s, h], z_recv.at[kind, s, h],
            device_id=(inner, blk), device_id_type=MESH,
        )

    def copy_out(s, h):
        return pltpu.make_async_remote_copy(
            rz.at[1, s, h], rz.at[1, s, h], b_send.at[s, h], z_recv.at[1, s, h],
            device_id=(outer, blk), device_id_type=MESH,
        )

    def copy_far(s, h):
        return pltpu.make_async_remote_copy(
            rz.at[1, s, h], tile.at[blk, h], b_send.at[s, h], p_recv.at[blk, h],
            device_id=(outer, s), device_id_type=MESH,
        )

    def arrived(k, s, h):
        return pltpu.make_async_remote_copy(
            rz.at[k, s, h], rz.at[k, s, h], a_send.at[s, h], z_recv.at[k, s, h],
            device_id=(inner, blk), device_id_type=MESH,
        )

    def copy_tile(s, h):
        return pltpu.make_async_remote_copy(
            rz.at[1, s, h], tile.at[blk, h], p_send.at[s, h], p_recv.at[blk, h],
            device_id=(grp, s), device_id_type=MESH,
        )

    def tile_wait(k, c):
        j = partner(blk, k, n_blk)
        for h in range(parts):
            pltpu.make_async_remote_copy(
                rz.at[1, j, h], tile.at[j, h], p_send.at[j, h], p_recv.at[j, h],
                device_id=(grp, j), device_id_type=MESH,
            ).wait_recv()
        return c

    def copy_dir(j):
        return pltpu.make_async_remote_copy(
            dirs.at[j], ret.at[blk], d_send.at[j], d_recv.at[blk],
            device_id=(grp, j), device_id_type=MESH,
        )

    def copy_stat(j):
        return pltpu.make_async_remote_copy(
            st_out, st_in.at[blk], s_send.at[j], s_recv.at[blk],
            device_id=(grp, j), device_id_type=MESH,
        )

    def stat_start(k, c):
        copy_stat(partner(blk, k, n_blk)).start()
        return c

    def dir_start(k, c):
        copy_dir(partner(blk, n_blk - k, n_blk)).start()
        return c

    def apply():
        lax.fori_loop(1, n_blk, tile_wait, 0)

        @pl.when(leaf)
        def _():
            tile_wait(0, 0)

        w_copies[0].wait()
        w_copies[1].wait()
        mine = tile[...].reshape(n_blk * rows, block)
        halfway = jnp.dot(rl[...], mine, preferred_element_type=jnp.float32).astype(jnp.bfloat16)
        direction = jnp.dot(halfway, rr[...], preferred_element_type=jnp.float32)
        dirs[...] = direction.astype(dirs.dtype).reshape(n_blk, rows, block)
        wide = mine.astype(jnp.float32)
        own_sq = jnp.sum(wide * wide)
        dir_sq = jnp.sum(direction * direction)
        row_id = lax.broadcasted_iota(jnp.int32, st_out.shape, 0)
        stats = jnp.where(row_id == 0, own_sq, dir_sq)
        st_out[...] = stats
        st_in[blk] = stats
        lax.fori_loop(1, n_blk, stat_start, 0)
        lax.fori_loop(1, n_blk, dir_start, 0)
        ret[blk] = dirs[blk]

    def phase(t, c):
        @pl.when(t < units)
        def _():
            s, h = target(t)
            b = n_tiles
            for i in range(n_tiles):
                b = jnp.where(slot_ref[i] == s, i, b)

            @pl.when(is_end)
            def _():
                snd[s, h] = xb[b, h]

            @pl.when(jnp.logical_not(is_end))
            def _():
                arrived(0, s, h).wait_recv()
                total = xb[b, h].astype(jnp.float32) + rz[0, s, h].astype(jnp.float32)
                snd[s, h] = total.astype(snd.dtype)

            copy_in(s, h).start()

        @pl.when(jnp.logical_and(jnp.logical_not(leaf), jnp.logical_and(t >= lag, t < units + lag)))
        def _():
            s, h = target(t - lag)
            arrived(1, s, h).wait_recv()

            @pl.when(is_mid)
            def _():
                total = snd[s, h].astype(jnp.float32) + rz[1, s, h].astype(jnp.float32)
                rz[1, s, h] = total.astype(rz.dtype)

            @pl.when(feeder)
            def _():
                copy_far(s, h).start()

            @pl.when(jnp.logical_not(jnp.logical_or(is_end, feeder)))
            def _():
                copy_out(s, h).start()

            @pl.when(s != blk)
            def _():
                copy_tile(s, h).start()

            @pl.when(s == blk)
            def _():
                tile[blk, h] = rz[1, blk, h]

        @pl.when(t == moment)
        def _():
            apply()

        return c

    lax.fori_loop(0, 2 * units + 1, phase, 0)
    owned = tile[...].reshape(n_blk * rows, block)
    nl_ref[0] = lax.dot_general(
        owned, owned, (((1,), (1,)), ((), ())), preferred_element_type=jnp.float32
    )
    nr_ref[0] = lax.dot_general(
        owned, owned, (((0,), (0,)), ((), ())), preferred_element_type=jnp.float32
    )

    def stat_wait(k, c):
        j = partner(blk, k, n_blk)
        pltpu.make_async_remote_copy(
            st_out, st_in.at[j], s_send.at[j], s_recv.at[j],
            device_id=(grp, j), device_id_type=MESH,
        ).wait()
        return c

    lax.fori_loop(1, n_blk, stat_wait, 0)
    squares = jnp.zeros((1, st_out.shape[1]), jnp.float32)
    for j in range(n_blk):
        squares = squares + st_in[j, 0:1, :]
    norm_factor = math.sqrt(block * n_tiles * block) / jnp.sqrt(squares)
    for j in range(n_blk):
        scales[j] = norm_factor * jnp.sqrt(st_in[j, 0:1, :]) / jnp.sqrt(st_in[j, 1:2, :] + 1e-6)
    gain = (1.0 - beta_two) * (norm_factor * norm_factor)[:, 0:1]
    w_copies[2].wait()
    w_copies[3].wait()
    nl_ref[0] = beta_two * sl[...] + gain * nl_ref[0]
    nr_ref[0] = beta_two * sr[...] + gain * nr_ref[0]

    def dir_wait(k, c):
        j = partner(blk, k, n_blk)
        pltpu.make_async_remote_copy(
            dirs.at[j], ret.at[j], d_send.at[j], d_recv.at[j],
            device_id=(grp, j), device_id_type=MESH,
        ).wait()
        return c

    lax.fori_loop(1, n_blk, dir_wait, 0)
    for b in range(n_tiles):
        s = slot_ref[b]
        up_ref[:, b * block : (b + 1) * block] = (
            ret[s].astype(jnp.float32) * scales[s][:, 0:1]
        ).astype(up_ref.dtype)

    def drain(s, c):
        for h in range(parts):
            copy_in(s, h).wait_send()

        @pl.when(jnp.logical_not(is_end))
        def _():
            for h in range(parts):
                copy_out(s, h).wait_send()

        @pl.when(jnp.logical_and(s != blk, jnp.logical_not(leaf)))
        def _():
            for h in range(parts):
                copy_tile(s, h).wait_send()

        return c

    lax.fori_loop(0, n_blk, drain, 0)


def writer(*refs):
    count = len(refs) // 2
    sources, targets, sems = refs[:count], refs[count:-1], refs[-1]
    copies = [
        pltpu.make_async_copy(src, dst, sems.at[i])
        for i, (src, dst) in enumerate(zip(sources, targets))
    ]
    for c in copies:
        c.start()
    for c in copies:
        c.wait()


def shards(n_grp, n_blk, partials, slot_of_block, stat_left, stat_right, root_left, root_right):
    rows, cols = partials.shape[1], partials.shape[2]
    block = stat_left.shape[1]
    n_tiles = cols // block
    vmem = pltpu.VMEM
    dma = pltpu.SemaphoreType.DMA
    half, single = jnp.bfloat16, jnp.float32
    hbm_spec = pl.BlockSpec(memory_space=pltpu.HBM)
    vmem_spec = pl.BlockSpec(memory_space=vmem)
    parts = 2 if rows % 32 == 0 else 1
    slots = (n_blk, rows, block)
    pieces = (parts, rows // parts, block)
    results = (
        ((1, block, block), single),
        ((1, block, block), single),
        ((rows, cols), half),
    )
    held_bytes = sum(math.prod(shape) * jnp.dtype(dtype).itemsize for shape, dtype in results)
    held = pl.pallas_call(
        functools.partial(kernel, n_grp, n_blk),
        out_shape=tuple(vmem(shape, dtype) for shape, dtype in results),
        in_specs=[pl.BlockSpec(memory_space=pltpu.SMEM)] + [hbm_spec] * 5,
        out_specs=(vmem_spec,) * 3,
        scratch_shapes=[
            vmem((n_tiles + 1, *pieces), half),
            vmem((n_blk, *pieces), half),
            vmem((2, n_blk, *pieces), half),
            vmem((n_blk, *pieces), half),
            vmem(slots, half),
            vmem(slots, half),
            vmem((8, 128), single),
            vmem((n_blk, 8, 128), single),
            vmem((n_blk, 1, 128), single),
            vmem((block, block), single),
            vmem((block, block), single),
            vmem((block, block), half),
            vmem((block, block), half),
            dma((n_tiles, parts)),
            dma((4,)),
            dma((n_blk, parts)),
            dma((2, n_blk, parts)),
            dma((n_blk, parts)),
            dma((n_blk, parts)),
            dma((n_blk, parts)),
            dma((n_blk,)),
            dma((n_blk,)),
            dma((n_blk,)),
            dma((n_blk,)),
        ],
        compiler_params=pltpu.CompilerParams(
            collective_id=0, has_side_effects=True, vmem_limit_bytes=vmem_bytes - held_bytes
        ),
        name="shampoo",
    )(slot_of_block, partials, stat_left, stat_right, root_left, root_right)
    return pl.pallas_call(
        writer,
        out_shape=tuple(jax.ShapeDtypeStruct(shape, dtype) for shape, dtype in results),
        in_specs=[vmem_spec] * 3,
        out_specs=(hbm_spec,) * 3,
        scratch_shapes=[dma((3,))],
        compiler_params=pltpu.CompilerParams(vmem_limit_bytes=2**20),
        name="writer",
    )(*held)


def solution(mesh):
    return jax.shard_map(
        functools.partial(shards, mesh.shape["grp"], mesh.shape["blk"]),
        mesh=mesh,
        in_specs=(
            P("grp", "blk", None),
            P(),
            P("blk", None, None),
            P("blk", None, None),
            P("blk", None, None),
            P("blk", None, None),
        ),
        out_specs=(P("blk", None, None), P("blk", None, None), P("blk", None)),
        check_vma=False,
    )
```
